8 devices in a mesh: dp: 1 (over z), tp: 2 (over y), ep: 4 (over x, core).
Axes of the slice: x: 2, y: 2, z: 1, core: 2. Of those that a mesh axis runs over, the one named last changes fastest.
Arguments:
- x: bfloat16 [4096, 2048], P(('dp', 'ep', 'tp'))
- idx: int32 [4096, 8], P(('dp', 'ep', 'tp'))
- gate: float32 [4096, 8], P(('dp', 'ep', 'tp'))
- w1: bfloat16 [64, 2048, 1024], P('ep', None, 'tp')
- w3: bfloat16 [64, 2048, 1024], P('ep', None, 'tp')
- w2: bfloat16 [64, 1024, 2048], P('ep', 'tp')
Outputs:
- output: bfloat16 [4096, 2048], P(('dp', 'ep', 'tp'))
All inputs are finite; a program needn't handle non-finite values.
Results may differ from the reference program's by a relative error of at most 0.001.
Values are sent between devices in bfloat16 or wider.
A program may use at most 1 GiB of HBM per device.

```python
import jax
import jax.numpy as jnp
from jax import lax

D = 2048
FF = 1024
EXPERTS = 64
TOP = 8
TOKENS_DEV = 512
EP = 4
TP = 2

ROWS = TOKENS_DEV * EP * TP
CAP = 8 * ((TOP * ROWS // EXPERTS + 9) // 8)


def _route(key):
    ndev = EP * TP
    nb = TOKENS_DEV // EP
    m = EXPERTS // EP
    k1 = (TOP + 1) // 2
    k2 = TOP - k1
    ka, kd, kt1, kt2, ks = jax.random.split(key, 5)
    a = jnp.argsort(jax.random.uniform(ka, (ndev, nb, EP)), axis=-1).astype(jnp.int32)
    shift = jax.random.randint(kd, (ndev, nb, 1), 1, EP)
    b = (a + shift) % EP
    r = (jnp.arange(ndev)[:, None] * nb + jnp.arange(nb)[None, :])[:, :, None]
    tau1 = jax.random.randint(kt1, (EP,), 0, m)
    tau2 = jax.random.randint(kt2, (EP,), 0, m)
    c1 = (r * k1 + tau1[a]) % m
    c2 = (r * k2 + tau2[b]) % m
    e1 = a[..., None] * m + (c1[..., None] + jnp.arange(k1)) % m
    e2 = b[..., None] * m + (c2[..., None] + jnp.arange(k2)) % m
    idx = jnp.concatenate([e1, e2], axis=-1).reshape(ROWS, TOP)
    perm = jnp.argsort(jax.random.uniform(ks, (ROWS, TOP)), axis=-1)
    return jnp.take_along_axis(idx, perm, axis=1).astype(jnp.int32)


def _weights(key, shape, fan_in):
    keys = jax.random.split(key, EXPERTS)
    return lax.map(lambda k: (jax.random.normal(k, shape, jnp.float32) * fan_in ** -0.5).astype(jnp.bfloat16), keys)


def setup_inputs(seed: int = 0, part: int = 0) -> dict:
    key = jax.random.PRNGKey(seed)
    k_shared, k_part = jax.random.split(key)
    kx, kr, kg = jax.random.split(jax.random.fold_in(k_part, part), 3)
    k1, k3, k2 = jax.random.split(k_shared, 3)
    x = jax.random.normal(kx, (ROWS, D), jnp.float32).astype(jnp.bfloat16)
    idx = _route(kr)
    gate = jax.nn.softmax(0.5 * jax.random.normal(kg, (ROWS, TOP), jnp.float32), axis=-1)
    return {'x': x, 'idx': idx, 'gate': gate,
            'w1': _weights(k1, (D, FF), D), 'w3': _weights(k3, (D, FF), D), 'w2': _weights(k2, (FF, D), FF)}


def reference(x, idx, gate, w1, w3, w2):
    flat = idx.reshape(-1)
    gflat = gate.reshape(-1)
    order = jnp.argsort(flat)
    counts = jnp.zeros((EXPERTS,), jnp.int32).at[flat].add(1)
    starts = jnp.cumsum(counts) - counts
    slot = jnp.arange(CAP)

    def body(acc, e_in):
        w1e, w3e, w2e, start, count = e_in
        pid = order[jnp.clip(start + slot, 0, flat.shape[0] - 1)]
        tok = pid // TOP
        g = jnp.where(slot < count, gflat[pid], 0.0)
        xe = x[tok]
        a = jnp.dot(xe, w1e, preferred_element_type=jnp.float32)
        b = jnp.dot(xe, w3e, preferred_element_type=jnp.float32)
        h = (jax.nn.silu(a) * b).astype(jnp.bfloat16)
        o = jnp.dot(h, w2e, preferred_element_type=jnp.float32)
        return acc.at[tok].add(o * g[:, None]), None

    acc, _ = lax.scan(body, jnp.zeros((ROWS, D), jnp.float32), (w1, w3, w2, starts, counts))
    return acc.astype(jnp.bfloat16)
```

```python
import functools

import jax
import jax.numpy as jnp
from jax import lax
from jax.experimental import pallas as pl
from jax.experimental.pallas import tpu as pltpu
from jax.sharding import PartitionSpec as P

PARTS = 2
BLOCK = 288
LO = 32


def _experts_kernel(slots, rows, cnt_ref, tok_ref, gate_ref, x_ref, w1_ref, w3_ref, w2_ref,
                    out_ref, acc_ref, xg_ref, o_ref, sem):
    e = pl.program_id(0)
    n = cnt_ref[e]
    chunks = x_ref.shape[1]
    half = chunks // 2

    @pl.when(e == 0)
    def _():
        def clear(i, _):
            b = pl.multiple_of(i * 8, 8)
            acc_ref[pl.ds(b, 8)] = jnp.zeros((8,) + acc_ref.shape[1:], jnp.float32)
            return 0
        lax.fori_loop(0, acc_ref.shape[0] // 8, clear, 0)

    def block(j, _):
        first = j * BLOCK
        base = e * slots + first
        left = jnp.minimum(n - first, BLOCK)

        def gather(i, _):
            b = pl.multiple_of(i * 16, 16)
            v = jnp.stack([x_ref[tok_ref[base + b + r]] for r in range(16)])
            v = jnp.swapaxes(v, 0, 1)
            for k in range(chunks):
                xg_ref[pl.ds(b, 16), k * 128:(k + 1) * 128] = v[k]
            return 0
        lax.fori_loop(0, (left + 15) // 16, gather, 0)

        xg = xg_ref[...]
        a = jnp.dot(xg, w1_ref[0], preferred_element_type=jnp.float32)
        b = jnp.dot(xg, w3_ref[0], preferred_element_type=jnp.float32)
        h = (jax.nn.silu(a) * b).astype(jnp.bfloat16)
        o_ref[...] = jnp.dot(h, w2_ref[0], preferred_element_type=jnp.float32)

        def scatter(i, _):
            b = pl.multiple_of(i * 8, 8)
            v = [jnp.swapaxes(jnp.stack([o_ref[pl.ds(b, 8), k * 128:(k + 1) * 128]
                                         for k in range(s * half, (s + 1) * half)]), 0, 1) for s in range(2)]
            for r in range(8):
                t = tok_ref[base + b + r]
                g = gate_ref[e * rows + t]
                t = jnp.where(b + r < left, t, rows)
                for s in range(2):
                    sl = slice(s * half, (s + 1) * half)
                    acc_ref[t, sl] = acc_ref[t, sl] + v[s][r] * g
            return 0
        lax.fori_loop(0, (left + 7) // 8, scatter, 0)
        return 0

    lax.fori_loop(0, (n + BLOCK - 1) // BLOCK, block, 0)

    @pl.when(e == pl.num_programs(0) - 1)
    def _():
        copy = pltpu.make_async_copy(acc_ref.at[pl.ds(0, rows)], out_ref, sem)
        copy.start()
        copy.wait()


def _experts(cnt, tok, ge, x3, w1, w3, w2):
    n_exp, d, f = w1.shape
    rows, chunks, lanes = x3.shape
    slots = tok.shape[1]
    once = pl.Buffered(1)
    return pl.pallas_call(
        functools.partial(_experts_kernel, slots, rows),
        grid_spec=pltpu.PrefetchScalarGridSpec(
            num_scalar_prefetch=3, grid=(n_exp,),
            in_specs=[pl.BlockSpec((rows, chunks, lanes), lambda e, *_: (0, 0, 0), pipeline_mode=once),
                      pl.BlockSpec((1, d, f), lambda e, *_: (e, 0, 0)),
                      pl.BlockSpec((1, d, f), lambda e, *_: (e, 0, 0)),
                      pl.BlockSpec((1, f, d), lambda e, *_: (e, 0, 0))],
            out_specs=pl.BlockSpec(memory_space=pl.ANY),
            scratch_shapes=[pltpu.VMEM((rows + 8, chunks, lanes), jnp.float32),
                            pltpu.VMEM((BLOCK, d), jnp.bfloat16),
                            pltpu.VMEM((BLOCK, d), jnp.float32),
                            pltpu.SemaphoreType.DMA]),
        out_shape=jax.ShapeDtypeStruct((rows, chunks, lanes), jnp.float32),
        compiler_params=pltpu.CompilerParams(vmem_limit_bytes=60 << 20),
        cost_estimate=pl.CostEstimate(flops=6 * n_exp * BLOCK * d * f, transcendentals=n_exp * BLOCK * f,
                                      bytes_accessed=6 * n_exp * d * f + 6 * rows * d),
        name='experts',
    )(cnt, tok.reshape(-1), ge.reshape(-1), x3, w1, w3, w2)


def _lists(idx_t, gate_t, lo, n_exp, slots):
    parts, _, rows = idx_t.shape
    bf, f32 = jnp.bfloat16, jnp.float32
    e = lo + jnp.arange(n_exp, dtype=jnp.int32)
    hit = idx_t[:, None] == e[None, :, None, None]
    mask = jnp.any(hit, axis=2)
    ge = jnp.sum(jnp.where(hit, gate_t[:, None], 0.0), axis=2)
    blk = mask.reshape(parts, n_exp, rows // 128, 128).astype(bf)
    i = jnp.arange(128)
    within = jnp.einsum('pent,ts->pens', blk, (i[:, None] < i[None, :]).astype(bf), preferred_element_type=f32)
    tot = jnp.sum(blk.astype(f32), axis=-1)
    m = jnp.arange(rows // 128)
    before = jnp.einsum('pen,nm->pem', tot.astype(bf), (m[:, None] < m[None, :]).astype(bf), preferred_element_type=f32)
    pos = (within + before[..., None]).reshape(parts, n_exp, rows).astype(jnp.int32)
    cnt = jnp.sum(tot, axis=-1).astype(jnp.int32)
    t = jnp.arange(rows, dtype=jnp.int32)
    hi = jnp.where(mask, pos // LO, -1)[:, :, None] == jnp.arange(slots // LO)[None, None, :, None]
    low = ((pos % LO)[:, :, None] == jnp.arange(LO)[None, None, :, None]).astype(bf)
    put = lambda v: jnp.einsum('peqt,pelt->peql', jnp.where(hi, v.astype(bf), 0), low, preferred_element_type=f32)
    tok = (put(t // 256) * 256 + put(t % 256)).astype(jnp.int32)
    return cnt, tok.reshape(parts, n_exp, slots), ge


def solution(mesh):
    rows_spec = P(('dp', 'ep', 'tp'), None)
    group = ('ep', 'tp')

    def body(x, idx, gate, w1, w3, w2):
        rows, d = x.shape
        n_exp, k = w1.shape[0], idx.shape[1]
        r = rows // PARTS
        x3 = x.reshape(rows, d // 128, 128)
        xa = [lax.all_gather(x3[p * r:(p + 1) * r], group, axis=0, tiled=True) for p in range(PARTS)]
        meta = jnp.concatenate([idx.astype(jnp.float32), gate], axis=1)
        meta = meta.reshape(PARTS, r, 2 * k).transpose(0, 2, 1)
        ma = lax.all_gather(meta, group, axis=2, tiled=True)
        lo = lax.axis_index('ep') * n_exp
        total = ma.shape[2]
        slots = BLOCK * (-(-min(520, total) // BLOCK))
        cnt, tok, ge = _lists(ma[:, :k].astype(jnp.int32), ma[:, k:], lo, n_exp, slots)
        outs = []
        for p in range(PARTS):
            part = _experts(cnt[p], tok[p], ge[p], xa[p], w1, w3, w2)
            outs.append(lax.psum_scatter(part, group, scatter_dimension=0, tiled=True))
        return jnp.concatenate([o.astype(jnp.bfloat16) for o in outs], axis=0).reshape(rows, d)

    return jax.shard_map(body, mesh=mesh,
                         in_specs=(rows_spec, rows_spec, rows_spec,
                                   P('ep', None, 'tp'), P('ep', None, 'tp'), P('ep', 'tp', None)),
                         out_specs=rows_spec, check_vma=False)
```

```python
import functools

import jax
import jax.numpy as jnp
from jax import lax
from jax.experimental import pallas as pl
from jax.experimental.pallas import tpu as pltpu
from jax.sharding import Mesh, PartitionSpec as P


PARTS = 4
BLOCK = 160
LO = 32


def _experts_kernel(slots, rows, cnt_ref, tok_ref, gate_ref, core_ref, x_ref, w1_ref, w3_ref, w2_ref,
                    own_ref, other_ref, acc_ref, xg_ref, o_ref, sem):
    e = pl.program_id(0)
    n = cnt_ref[e]
    chunks = x_ref.shape[1]
    half = chunks // 2

    @pl.when(e == 0)
    def _():
        def clear(i, _):
            b = pl.multiple_of(i * 8, 8)
            acc_ref[pl.ds(b, 8)] = jnp.zeros((8,) + acc_ref.shape[1:], jnp.float32)
            return 0
        lax.fori_loop(0, acc_ref.shape[0] // 8, clear, 0)

    def block(j, _):
        first = j * BLOCK
        base = e * slots + first
        left = jnp.minimum(n - first, BLOCK)

        def gather(i, _):
            b = pl.multiple_of(i * 16, 16)
            v = jnp.stack([x_ref[tok_ref[base + b + r]] for r in range(16)])
            v = jnp.swapaxes(v, 0, 1)
            for k in range(chunks):
                xg_ref[pl.ds(b, 16), k * 128:(k + 1) * 128] = v[k]
            return 0
        lax.fori_loop(0, (left + 15) // 16, gather, 0)

        xg = xg_ref[...]
        a = jnp.dot(xg, w1_ref[0], preferred_element_type=jnp.float32)
        b = jnp.dot(xg, w3_ref[0], preferred_element_type=jnp.float32)
        h = (jax.nn.silu(a) * b).astype(jnp.bfloat16)
        o_ref[...] = jnp.dot(h, w2_ref[0], preferred_element_type=jnp.float32)

        def scatter(i, _):
            b = pl.multiple_of(i * 8, 8)
            v = [jnp.swapaxes(jnp.stack([o_ref[pl.ds(b, 8), k * 128:(k + 1) * 128]
                                         for k in range(s * half, (s + 1) * half)]), 0, 1) for s in range(2)]
            for r in range(8):
                t = tok_ref[base + b + r]
                g = gate_ref[e * rows + t]
                t = jnp.where(b + r < left, t, rows)
                for s in range(2):
                    sl = slice(s * half, (s + 1) * half)
                    acc_ref[t, sl] = acc_ref[t, sl] + v[s][r] * g
            return 0
        lax.fori_loop(0, (left + 7) // 8, scatter, 0)
        return 0

    lax.fori_loop(0, (n + BLOCK - 1) // BLOCK, block, 0)

    @pl.when(e == pl.num_programs(0) - 1)
    def _():
        c = core_ref[0]
        q = rows // 4
        copies = []
        for i in range(2):
            for ref, core in ((other_ref, 1 - c), (own_ref, c)):
                src = acc_ref.at[pl.ds(pl.multiple_of((2 * i + core) * q, q), q)]
                copies.append(pltpu.make_async_copy(src, ref.at[pl.ds(i * q, q)], sem.at[len(copies)]))
        for copy in copies:
            copy.start()
        for copy in copies:
            copy.wait()


def _experts(cnt, tok, ge, core, x3, w1, w3, w2):
    n_exp, d, f = w1.shape
    rows, chunks, lanes = x3.shape
    slots = tok.shape[1]
    once = pl.Buffered(1)
    return pl.pallas_call(
        functools.partial(_experts_kernel, slots, rows),
        grid_spec=pltpu.PrefetchScalarGridSpec(
            num_scalar_prefetch=4, grid=(n_exp,),
            in_specs=[pl.BlockSpec((rows, chunks, lanes), lambda e, *_: (0, 0, 0), pipeline_mode=once),
                      pl.BlockSpec((1, d, f), lambda e, *_: (e, 0, 0)),
                      pl.BlockSpec((1, d, f), lambda e, *_: (e, 0, 0)),
                      pl.BlockSpec((1, f, d), lambda e, *_: (e, 0, 0))],
            out_specs=[pl.BlockSpec(memory_space=pl.ANY)] * 2,
            scratch_shapes=[pltpu.VMEM((rows + 8, chunks, lanes), jnp.float32),
                            pltpu.VMEM((BLOCK, d), jnp.bfloat16),
                            pltpu.VMEM((BLOCK, d), jnp.float32),
                            pltpu.SemaphoreType.DMA((4,))]),
        out_shape=[jax.ShapeDtypeStruct((rows // 2, chunks, lanes), jnp.float32)] * 2,
        compiler_params=pltpu.CompilerParams(vmem_limit_bytes=60 << 20),
        cost_estimate=pl.CostEstimate(flops=6 * n_exp * BLOCK * d * f, transcendentals=n_exp * BLOCK * f,
                                      bytes_accessed=6 * n_exp * d * f + 6 * rows * d),
        name='experts',
    )(cnt, tok.reshape(-1), ge.reshape(-1), core, x3, w1, w3, w2)


def _lists(idx_t, gate_t, lo, n_exp, slots):
    parts, _, rows = idx_t.shape
    bf, f32 = jnp.bfloat16, jnp.float32
    e = lo + jnp.arange(n_exp, dtype=jnp.int32)
    hit = idx_t[:, None] == e[None, :, None, None]
    mask = jnp.any(hit, axis=2)
    ge = jnp.sum(jnp.where(hit, gate_t[:, None], 0.0), axis=2)
    blk = mask.reshape(parts, n_exp, rows // 128, 128).astype(bf)
    i = jnp.arange(128)
    within = jnp.einsum('pent,ts->pens', blk, (i[:, None] < i[None, :]).astype(bf), preferred_element_type=f32)
    tot = jnp.sum(blk.astype(f32), axis=-1)
    m = jnp.arange(rows // 128)
    before = jnp.einsum('pen,nm->pem', tot.astype(bf), (m[:, None] < m[None, :]).astype(bf), preferred_element_type=f32)
    pos = (within + before[..., None]).reshape(parts, n_exp, rows).astype(jnp.int32)
    cnt = jnp.sum(tot, axis=-1).astype(jnp.int32)
    t = jnp.arange(rows, dtype=jnp.int32)
    hi = jnp.where(mask, pos // LO, -1)[:, :, None] == jnp.arange(slots // LO)[None, None, :, None]
    low = ((pos % LO)[:, :, None] == jnp.arange(LO)[None, None, :, None]).astype(bf)
    put = lambda v: jnp.einsum('peqt,pelt->peql', jnp.where(hi, v.astype(bf), 0), low, preferred_element_type=f32)
    tok = (put(t // 256) * 256 + put(t % 256)).astype(jnp.int32)
    return cnt, tok.reshape(parts, n_exp, slots), ge


def solution(mesh):
    dp, tp, ep = (mesh.shape[a] for a in ('dp', 'tp', 'ep'))
    mesh = Mesh(mesh.devices.reshape(dp, tp, ep // 2, 2), ('dp', 'tp', 'x', 'core'))
    rows_spec = P(('dp', 'x', 'core', 'tp'), None)
    group = ('x', 'core', 'tp')

    def body(x, idx, gate, w1, w3, w2):
        rows, d = x.shape
        n_exp, k = w1.shape[0], idx.shape[1]
        r = rows // PARTS
        x3 = x.reshape(rows, d // 128, 128)
        xa = [lax.all_gather(x3[p * r:(p + 1) * r], group, axis=0, tiled=True) for p in range(PARTS)]
        meta = jnp.concatenate([idx.astype(jnp.float32), gate], axis=1)
        meta = meta.reshape(PARTS, r, 2 * k).transpose(0, 2, 1)
        ma = lax.all_gather(meta, group, axis=2, tiled=True)
        core = lax.axis_index('core')
        lo = (lax.axis_index('x') * 2 + core) * n_exp
        total = ma.shape[2]
        slots = BLOCK * (-(-min(520, total) // BLOCK))
        cnt, tok, ge = _lists(ma[:, :k].astype(jnp.int32), ma[:, k:], lo, n_exp, slots)
        outs = []
        for p in range(PARTS):
            own, other = _experts(cnt[p], tok[p], ge[p], core.reshape(1), xa[p], w1, w3, w2)
            part = own + lax.ppermute(other, 'core', [(0, 1), (1, 0)])
            outs.append(lax.psum_scatter(part, ('x', 'tp'), scatter_dimension=0, tiled=True))
        return jnp.concatenate([o.astype(jnp.bfloat16) for o in outs], axis=0).reshape(rows, d)

    return jax.shard_map(body, mesh=mesh,
                         in_specs=(rows_spec, rows_spec, rows_spec,
                                   P(('x', 'core'), None, 'tp'), P(('x', 'core'), None, 'tp'),
                                   P(('x', 'core'), 'tp', None)),
                         out_specs=rows_spec, check_vma=False)
```

```python
import functools

import jax
import jax.numpy as jnp
from jax import lax
from jax.experimental import pallas as pl
from jax.experimental.pallas import tpu as pltpu
from jax.sharding import Mesh, PartitionSpec as P


SIZES = (12, 11, 9)
LO = 16


def _experts_kernel(block_rows, slots, rows, cnt_ref, tok_ref, gate_ref, core_ref, x_ref, w1_ref, w3_ref, w2_ref,
                    own_ref, other_ref, acc_ref, xg_ref, o_ref, sem):
    e = pl.program_id(0)
    n = cnt_ref[e]
    chunks = x_ref.shape[1]
    half = chunks // 2

    @pl.when(e == 0)
    def _():
        def clear(i, _):
            b = pl.multiple_of(i * 8, 8)
            acc_ref[pl.ds(b, 8)] = jnp.zeros((8,) + acc_ref.shape[1:], jnp.float32)
            return 0
        lax.fori_loop(0, acc_ref.shape[0] // 8, clear, 0)

    def block(j, _):
        first = j * block_rows
        base = e * slots + first
        left = jnp.minimum(n - first, block_rows)

        def gather(i, _):
            b = pl.multiple_of(i * 16, 16)
            v = jnp.stack([x_ref[tok_ref[base + b + r]] for r in range(16)])
            v = jnp.swapaxes(v, 0, 1)
            for k in range(chunks):
                xg_ref[pl.ds(b, 16), k * 128:(k + 1) * 128] = v[k]
            return 0
        lax.fori_loop(0, (left + 15) // 16, gather, 0)

        xg = xg_ref[...]
        a = jnp.dot(xg, w1_ref[0], preferred_element_type=jnp.float32)
        b = jnp.dot(xg, w3_ref[0], preferred_element_type=jnp.float32)
        h = (jax.nn.silu(a) * b).astype(jnp.bfloat16)
        o_ref[...] = jnp.dot(h, w2_ref[0], preferred_element_type=jnp.float32)

        def scatter(i, _):
            b = pl.multiple_of(i * 8, 8)
            v = [jnp.swapaxes(jnp.stack([o_ref[pl.ds(b, 8), k * 128:(k + 1) * 128]
                                         for k in range(s * half, (s + 1) * half)]), 0, 1) for s in range(2)]
            for r in range(8):
                t = tok_ref[base + b + r]
                g = gate_ref[e * rows + t]
                t = jnp.where(b + r < left, t, rows)
                for s in range(2):
                    sl = slice(s * half, (s + 1) * half)
                    acc_ref[t, sl] = acc_ref[t, sl] + v[s][r] * g
            return 0
        lax.fori_loop(0, (left + 7) // 8, scatter, 0)
        return 0

    lax.fori_loop(0, (n + block_rows - 1) // block_rows, block, 0)

    @pl.when(e == pl.num_programs(0) - 1)
    def _():
        c = core_ref[0]
        q = rows // 4
        copies = []
        for i in range(2):
            for ref, core in ((other_ref, 1 - c), (own_ref, c)):
                src = acc_ref.at[pl.ds(pl.multiple_of((2 * i + core) * q, q), q)]
                copies.append(pltpu.make_async_copy(src, ref.at[pl.ds(i * q, q)], sem.at[len(copies)]))
        for copy in copies:
            copy.start()
        for copy in copies:
            copy.wait()


def _experts(block_rows, cnt, tok, ge, core, x3, w1, w3, w2):
    n_exp, d, f = w1.shape
    rows, chunks, lanes = x3.shape
    slots = tok.shape[1]
    once = pl.Buffered(1)
    return pl.pallas_call(
        functools.partial(_experts_kernel, block_rows, slots, rows),
        grid_spec=pltpu.PrefetchScalarGridSpec(
            num_scalar_prefetch=4, grid=(n_exp,),
            in_specs=[pl.BlockSpec((rows, chunks, lanes), lambda e, *_: (0, 0, 0), pipeline_mode=once),
                      pl.BlockSpec((1, d, f), lambda e, *_: (e, 0, 0)),
                      pl.BlockSpec((1, d, f), lambda e, *_: (e, 0, 0)),
                      pl.BlockSpec((1, f, d), lambda e, *_: (e, 0, 0))],
            out_specs=[pl.BlockSpec(memory_space=pl.ANY)] * 2,
            scratch_shapes=[pltpu.VMEM((rows + 8, chunks, lanes), jnp.float32),
                            pltpu.VMEM((block_rows, d), jnp.bfloat16),
                            pltpu.VMEM((block_rows, d), jnp.float32),
                            pltpu.SemaphoreType.DMA((4,))]),
        out_shape=[jax.ShapeDtypeStruct((rows // 2, chunks, lanes), jnp.float32)] * 2,
        compiler_params=pltpu.CompilerParams(vmem_limit_bytes=60 << 20),
        cost_estimate=pl.CostEstimate(flops=6 * n_exp * block_rows * d * f, transcendentals=n_exp * block_rows * f,
                                      bytes_accessed=6 * n_exp * d * f + 6 * rows * d),
        name='experts',
    )(cnt, tok.reshape(-1), ge.reshape(-1), core, x3, w1, w3, w2)


def _lists(idx_t, gate_t, lo, n_exp, slots):
    parts, _, rows = idx_t.shape
    bf, f32 = jnp.bfloat16, jnp.float32
    e = lo + jnp.arange(n_exp, dtype=jnp.int32)
    hit = idx_t[:, None] == e[None, :, None, None]
    mask = jnp.any(hit, axis=2)
    ge = jnp.sum(jnp.where(hit, gate_t[:, None], 0.0), axis=2)
    blk = mask.reshape(parts, n_exp, rows // 128, 128).astype(bf)
    i = jnp.arange(128)
    within = jnp.einsum('pent,ts->pens', blk, (i[:, None] < i[None, :]).astype(bf), preferred_element_type=f32)
    tot = jnp.sum(blk.astype(f32), axis=-1)
    m = jnp.arange(rows // 128)
    before = jnp.einsum('pen,nm->pem', tot.astype(bf), (m[:, None] < m[None, :]).astype(bf), preferred_element_type=f32)
    pos = (within + before[..., None]).reshape(parts, n_exp, rows).astype(jnp.int32)
    cnt = jnp.sum(tot, axis=-1).astype(jnp.int32)
    t = jnp.arange(rows, dtype=jnp.int32)
    hi = jnp.where(mask, pos // LO, -1)[:, :, None] == jnp.arange(slots // LO)[None, None, :, None]
    low = ((pos % LO)[:, :, None] == jnp.arange(LO)[None, None, :, None]).astype(bf)
    put = lambda v: jnp.einsum('peqt,pelt->peql', jnp.where(hi, v.astype(bf), 0), low, preferred_element_type=f32)
    tok = (put(t // 256) * 256 + put(t % 256)).astype(jnp.int32)
    return cnt, tok.reshape(parts, n_exp, slots), ge


def solution(mesh):
    dp, tp, ep = (mesh.shape[a] for a in ('dp', 'tp', 'ep'))
    mesh = Mesh(mesh.devices.reshape(dp, tp, ep // 2, 2), ('dp', 'tp', 'x', 'core'))
    rows_spec = P(('dp', 'x', 'core', 'tp'), None)
    group = ('x', 'core', 'tp')

    def body(x, idx, gate, w1, w3, w2):
        rows, d = x.shape
        n_exp, k = w1.shape[0], idx.shape[1]
        x3 = x.reshape(rows, d // 128, 128)
        cuts = [sum(SIZES[:i]) * rows // sum(SIZES) for i in range(len(SIZES) + 1)]
        xa = [lax.all_gather(x3[a:b], group, axis=0, tiled=True) for a, b in zip(cuts, cuts[1:])]
        meta = jnp.concatenate([idx.astype(jnp.float32), gate], axis=1).T
        ma = lax.all_gather(meta, group, axis=1, tiled=False)
        core = lax.axis_index('core')
        lo = (lax.axis_index('x') * 2 + core) * n_exp
        outs = []
        for p, (a, b) in enumerate(zip(cuts, cuts[1:])):
            block_rows = b - a + 32
            slots = block_rows * -(-520 // block_rows)
            mp = ma[:, :, a:b].reshape(1, 2 * k, -1)
            cnt, tok, ge = _lists(mp[:, :k].astype(jnp.int32), mp[:, k:], lo, n_exp, slots)
            own, other = _experts(block_rows, cnt[0], tok[0], ge[0], core.reshape(1), xa[p], w1, w3, w2)
            part = own + lax.ppermute(other, 'core', [(0, 1), (1, 0)])
            outs.append(lax.psum_scatter(part, ('x', 'tp'), scatter_dimension=0, tiled=True))
        return jnp.concatenate([o.astype(jnp.bfloat16) for o in outs], axis=0).reshape(rows, d)

    return jax.shard_map(body, mesh=mesh,
                         in_specs=(rows_spec, rows_spec, rows_spec,
                                   P(('x', 'core'), None, 'tp'), P(('x', 'core'), None, 'tp'),
                                   P(('x', 'core'), 'tp', None)),
                         out_specs=rows_spec, check_vma=False)
```
